32 devices in a mesh: seq: 8 (over y, x, core), head: 4 (over z).
Axes of the slice: x: 2, y: 2, z: 4, core: 2. Of those that a mesh axis runs over, the one named last changes fastest.
Arguments:
- span_order: int32 [16], replicated, may hold values from 0 to 15, each once
- queries: bfloat16 [1024, 36864], P('seq', 'head'), may hold values from -32 to 32
- latent_kv: bfloat16 [1024, 576], P(('seq', 'head')), may hold values from -8 to 8
- w_uv: bfloat16 [64, 512, 128], P('head'), may hold values from -0.25 to 0.25
Outputs:
- attended: bfloat16 [1024, 8192], P('seq', 'head')
The draws below stay inside these ranges and needn't reach their ends.
Inputs may be any that keep to these rules, and one draw needn't show every extreme that they name: `span_order`: each of 0 to 15 appears once.
All inputs are finite; a program needn't handle non-finite values.
Results may differ from the reference program's by a relative error of at most 0.0065.
Values may be sent and summed in bfloat16 or wider, within the bound.
A program may use at most 128 MiB of HBM per device.

```python
import math
import jax
import jax.numpy as jnp
from jax import lax

HEADS = 64
KV_RANK = 512
ROPE_DIM = 64
NOPE_DIM = 128
V_DIM = 128
QK_DIM = 576
TOK_DEV = 128
SEQS = 2
TOKENS = 1024
SEQ_LEN = 512
SPANS = 16


def draw_latent_kv(key, part):
    drawn = jnp.clip(jax.random.normal(jax.random.fold_in(key, 1), (TOKENS, QK_DIM), jnp.float32), -6.0, 6.0)
    return drawn.astype(jnp.bfloat16)


def draw_queries(key, part):
    drawn = jnp.clip(jax.random.normal(jax.random.fold_in(key, 21), (TOKENS, HEADS, QK_DIM), jnp.float32), -6.0, 6.0)
    return drawn.reshape(TOKENS, HEADS * QK_DIM).astype(jnp.bfloat16)


def levels(rng, extent, split, low, high):
    def one(position, blocks):
        draws = jax.random.uniform(jax.random.fold_in(jax.random.fold_in(rng, 6), position), (blocks,), jnp.float32, low / len(split), high / len(split))
        return jnp.repeat(jnp.exp(draws), extent[position] // blocks).reshape((-1,) + (1,) * (len(extent) - position - 1))

    factor_of = one(*split[0])
    for cut in split[1:]:
        factor_of = factor_of * one(*cut)
    return factor_of


def noise(own_key, shape, spread, reach, pieces=(), kind=jnp.bfloat16):
    values = spread * jax.random.normal(own_key, shape, jnp.float32)
    if pieces:
        values = values * levels(own_key, shape, pieces, -0.22, 0.18)
    return jnp.clip(values, -reach, reach).astype(kind)


def setup_inputs(seed: int = 0) -> dict:
    arg_keys = jax.random.split(jax.random.key(seed), 5)
    return {
        "span_order": jax.random.permutation(arg_keys[0], SPANS).astype(jnp.int32),
        "queries": draw_queries(jax.random.fold_in(arg_keys[4], 71), 0),
        "latent_kv": draw_latent_kv(jax.random.fold_in(arg_keys[4], 71), 0),
        "w_uv": noise(arg_keys[3], (HEADS, KV_RANK, V_DIM), KV_RANK ** -0.5, 0.25, ((0, 4),)),
    }


theta_base = 10000.0


def angle_tables(positions, half_width):
    inverse_freq = jnp.exp(-math.log(theta_base) * jnp.arange(half_width, dtype=jnp.float32) / half_width)
    phases = positions.astype(jnp.float32)[:, None] * inverse_freq[None, :]
    return jnp.cos(phases), jnp.sin(phases)


def rotate(values, cosine, sine_table):
    half_width = values.shape[-1] // 2
    lower_part = values[..., :half_width]
    upper_part = values[..., half_width:]
    return jnp.concatenate([lower_part * cosine - upper_part * sine_table, upper_part * cosine + lower_part * sine_table], -1)


def reference(span_order, queries, latent_kv, w_uv):
    span_len = TOK_DEV // 2
    stream_ids = (span_order[:, None] * span_len + jnp.arange(span_len, dtype=jnp.int32)[None, :]).reshape(-1).astype(jnp.int32)
    positions = stream_ids % SEQ_LEN
    cosine, sine_table = angle_tables(positions, ROPE_DIM // 2)
    key_rows = jnp.concatenate([latent_kv[:, :KV_RANK], rotate(latent_kv[:, KV_RANK:].astype(jnp.float32), cosine, sine_table).astype(jnp.bfloat16)], 1)
    sorted_rows = jnp.argsort(stream_ids).astype(jnp.int32)
    ordered_key_rows = lax.optimization_barrier(key_rows[sorted_rows]).astype(jnp.float32).reshape(SEQS, SEQ_LEN, QK_DIM)
    ordered_value_rows = ordered_key_rows[..., :KV_RANK]
    query_grid = queries.reshape(TOKENS, HEADS, QK_DIM)
    causal = jnp.arange(SEQ_LEN)[:, None] >= jnp.arange(SEQ_LEN)[None, :]
    logit_scale_factor = (NOPE_DIM + ROPE_DIM) ** -0.5

    def one_head(head_index):
        query_head = lax.dynamic_index_in_dim(query_grid, head_index, 1, keepdims=False)
        rotated = rotate(query_head[:, KV_RANK:].astype(jnp.float32), cosine, sine_table).astype(jnp.bfloat16)
        query_head = jnp.concatenate([query_head[:, :KV_RANK], rotated], 1)
        ordered_query_rows = lax.optimization_barrier(query_head[sorted_rows]).astype(jnp.float32).reshape(SEQS, SEQ_LEN, QK_DIM)
        logit_scores = jnp.einsum("xpa,xfa->xpf", ordered_query_rows, ordered_key_rows) * logit_scale_factor
        logit_scores = jnp.where(causal[None], logit_scores, -jnp.inf)
        row_top = jnp.max(logit_scores, -1, keepdims=True)
        expo = jnp.exp(logit_scores - row_top)
        totals = jnp.sum(expo, -1)
        softmax_weights = lax.optimization_barrier(expo.astype(jnp.bfloat16)).astype(jnp.float32)
        numerator_sums = jnp.einsum("mzw,mwi->mzi", softmax_weights, ordered_value_rows)
        latent_out = lax.optimization_barrier((numerator_sums / totals[..., None]).astype(jnp.bfloat16)).astype(jnp.float32)
        weight_head = lax.dynamic_index_in_dim(w_uv, head_index, 0, keepdims=False).astype(jnp.float32)
        projected = jnp.einsum("bqr,rv->bqv", latent_out, weight_head).astype(jnp.bfloat16)
        return projected.reshape(TOKENS, V_DIM)[stream_ids]

    outputs = lax.map(one_head, jnp.arange(HEADS, dtype=jnp.int32))
    return jnp.moveaxis(outputs, 0, 1).reshape(TOKENS, HEADS * V_DIM)
```

```python
import functools
import math

import jax
import jax.numpy as jnp
import numpy as np
from jax import lax
from jax.experimental import pallas as pl
from jax.experimental.pallas import tpu as pltpu
from jax.sharding import PartitionSpec as P

ROPE_DIM = 64
NOPE_DIM = 128
SEQS = 2
LANES = 128
CHUNK_SPANS = 8
GATHER_MIB = 24
ATTEND_MIB = 40

theta_base = 10000.0
logit_scale = (NOPE_DIM + ROPE_DIM) ** -0.5


def angle_table(count, half):
    freq = np.exp(-math.log(theta_base) * np.arange(half, dtype=np.float32) / half).astype(
        np.float32
    )
    phases = (np.arange(count, dtype=np.float32)[:, None] * freq[None, :]).astype(np.float64)
    cosine, sine = np.cos(phases), np.sin(phases)
    return np.concatenate([cosine, cosine, -sine, sine], 1).astype(np.float32)


def flip(index, bits):
    out = index
    place = 1
    while place <= bits:
        if bits & place:
            out = out + place * (1 - 2 * ((index // place) % 2))
        place *= 2
    return out


def rotate_tile(tile, table, high):
    lane = lax.broadcasted_iota(jnp.int32, tile.shape, tile.ndim - 1)
    quarter = lane // (ROPE_DIM // 2)
    last = tile.ndim - 1
    forward = pltpu.roll(tile, ROPE_DIM // 2, last)
    backward = pltpu.roll(tile, LANES - ROPE_DIM // 2, last)
    swapped = jnp.where(quarter % 2 == 0, backward, forward)
    turned = pltpu.roll(table, ROPE_DIM, 1)
    cosine, sine = (turned, table) if high else (table, turned)
    here = (quarter >= 2) if high else (quarter < 2)
    return jnp.where(here, tile * cosine + swapped * sine, tile)


def span_places(order_ref, s, spans_seq, span_len):
    seq_first, place = [], []
    for span in range(2):
        mine = order_ref[2 * s + span]
        first = jnp.int32(0)
        for later in range(1, SEQS):
            first = jnp.where(mine >= later * spans_seq, later * spans_seq, first)
        seq_first.append(first)
        place.append((mine - first) * span_len)
    return seq_first, place


def gather_kernel(
    dims,
    latent_ref,
    kv,
    z_send,
    z_recv,
    p_send,
    p_recv,
    d_send,
    d_recv,
    ready,
):
    n_seq, n_head, heads, rank, span_len, kv_count, spans_seq = dims
    s = lax.axis_index("seq")
    h = lax.axis_index("head")
    far = range(2, n_seq, 2)
    mesh_id = pl.DeviceIdType.MESH
    barrier = pltpu.get_barrier_semaphore()
    peers = [(d, 0) for d in far] + [(0, k) for k in range(1, n_head)] + [(1, 0)]
    peers.sort(key=lambda peer: bin(peer[0]).count("1") + (peer[1] + peer[1] // 2) * 0.9)

    def signal(sem, d, k):
        pl.semaphore_signal(
            sem,
            inc=1,
            device_id={"seq": flip(s, d), "head": flip(h, k)},
            device_id_type=mesh_id,
        )

    def later(d, k):
        return flip(h, k) > h if k else flip(s, d) > s

    sent = []

    def describe(d, k, send, recv, to_d, to_k):
        block = kv.at[flip(s, d) * n_head + flip(h, k)]
        copy = pltpu.make_async_remote_copy(
            src_ref=block if d or k else latent_ref,
            dst_ref=block,
            send_sem=send,
            recv_sem=recv,
            device_id={"seq": flip(s, to_d), "head": flip(h, to_k)},
            device_id_type=mesh_id,
        )
        sent.append(copy)
        return copy

    def arrived(d, k, send, recv):
        block = kv.at[flip(s, d) * n_head + flip(h, k)]
        pltpu.make_async_remote_copy(
            src_ref=block,
            dst_ref=block,
            send_sem=send,
            recv_sem=recv,
            device_id={"seq": flip(s, 1), "head": h},
            device_id_type=mesh_id,
        ).wait_recv()

    before = jnp.int32(0)
    for peer in peers:
        before = before + jnp.where(later(*peer), 0, 1)

        @pl.when(later(*peer))
        def _(peer=peer):
            signal(barrier, *peer)

    kv[s * n_head + h] = latent_ref[...]

    @pl.when(before > 0)
    def _():
        pl.semaphore_wait(barrier, before)

    for i, peer in enumerate(peers):

        @pl.when(jnp.logical_not(later(*peer)))
        def _(i=i, peer=peer):
            signal(ready.at[i], *peer)

    first = []
    for d, k in peers:
        if k:
            first.append(describe(0, 0, z_send.at[k - 1], z_recv.at[k - 1], 0, k))
        elif d > 1:
            first.append(describe(0, 0, p_send.at[0, d // 2], p_recv.at[0, d // 2], d, 0))
        else:
            first.append(describe(0, 0, d_send.at[0, 0], d_recv.at[0, 0], 1, 0))
    for peer, copy in zip(peers, first):
        pl.when(jnp.logical_not(later(*peer)))(copy.start)
    for i, (peer, copy) in enumerate(zip(peers, first)):

        @pl.when(later(*peer))
        def _(i=i, copy=copy):
            pl.semaphore_wait(ready.at[i], 1)
            copy.start()

    def spread(k, d):
        if d == 0:
            for to in reversed(far):
                describe(0, k, p_send.at[k, to // 2], p_recv.at[k, to // 2], to, 0).start()
        describe(d, k, d_send.at[k, d // 2], d_recv.at[k, d // 2], 1, 0).start()

    events = []
    for k in range(n_head):
        for d in range(0, n_seq, 2):
            if d:
                events.append((k + bin(d).count("1") + 2, d, k))
            elif k:
                events.append((k, d, k))
    for _, d, k in sorted(events):
        if d:
            arrived(d, k, p_send.at[k, d // 2], p_recv.at[k, d // 2])
        else:
            arrived(0, k, z_send.at[k - 1], z_recv.at[k - 1])
        spread(k, d)
    for k in range(n_head):
        for d in range(0, n_seq, 2):
            arrived(d + 1, k, d_send.at[k, d // 2], d_recv.at[k, d // 2])
    for copy in sent:
        copy.wait_send()


def attend_kernel(
    dims, order_ref, queries_ref, kv, table, w_ref, out_ref, q_rows, keys, mixed, state
):
    n_seq, n_head, heads, rank, span_len, kv_count, spans_seq = dims
    width = rank + ROPE_DIM
    pairs = heads // 2
    s = lax.axis_index("seq")
    spans = SEQS * spans_seq
    per_span = span_len // kv_count
    seq_first, place = span_places(order_ref, s, spans_seq, span_len)
    for span in range(2):
        angles = table[pl.ds(place[span], span_len), :]
        for par in range(2):
            for pair in range(pairs):
                source = pl.ds(span * span_len, span_len)
                first = pair * 2 * width + par * rank
                rows = pl.ds(pair * span_len, span_len)
                tiles = [
                    queries_ref[source, pl.ds(first + c, LANES)] for c in range(0, rank + 1, LANES)
                ]
                tiles[-1] = rotate_tile(
                    tiles[-1].astype(jnp.float32), angles, bool(par)
                ).astype(jnp.bfloat16)
                q_rows[span, par, rows, :] = jnp.concatenate(tiles, 1)

    def block_of(stream_span):
        def pick(slot, found):
            return jnp.where(order_ref[slot] == stream_span, slot * per_span, found)

        if spans > 16:
            return lax.fori_loop(0, spans, pick, jnp.int32(0))
        found = jnp.int32(0)
        for slot in range(spans):
            found = pick(slot, found)
        return found

    chunk_spans = min(CHUNK_SPANS, spans_seq)
    n_chunks = spans_seq // chunk_spans
    chunk = chunk_spans * span_len

    for span in range(2):
        def one_chunk(c, span=span):
            for j in range(chunk_spans):
                block = block_of(seq_first[span] + c * chunk_spans + j)
                raw = kv[pl.ds(block, per_span)].reshape(span_len, width)
                angles = table[pl.ds((c * chunk_spans + j) * span_len, span_len), :]
                pad = jnp.zeros((span_len, LANES - ROPE_DIM), jnp.float32)
                rope = jnp.concatenate([raw[:, rank:].astype(jnp.float32), pad], 1)
                rope = rotate_tile(rope, angles, False)
                rows = pl.ds(j * span_len, span_len)
                keys[0, rows, :rank] = raw[:, :rank]
                keys[0, rows, rank:] = rope.astype(jnp.bfloat16)
                whole = jnp.concatenate([raw[:, :rank].astype(jnp.float32), rope], 1)
                keys[1, rows, :] = pltpu.roll(whole, ROPE_DIM, 1).astype(jnp.bfloat16)
            limit = lax.broadcasted_iota(jnp.int32, (span_len, chunk), 0) + place[span]
            seen = lax.broadcasted_iota(jnp.int32, (span_len, chunk), 1) + c * chunk <= limit
            for par in range(2):
                scores = (
                    lax.dot_general(
                        q_rows[span, par],
                        keys[par],
                        (((1,), (1,)), ((), ())),
                        preferred_element_type=jnp.float32,
                    )
                    * logit_scale
                )
                scores = jnp.where(
                    seen[None], scores.reshape(pairs, span_len, chunk), -jnp.inf
                ).reshape(pairs * span_len, chunk)
                top = jnp.max(scores, 1, keepdims=True)
                if n_chunks > 1:
                    old_top = state[par, :, 0:1]
                    top = jnp.maximum(top, old_top)
                    shrink = jnp.exp(old_top - top)
                expo = jnp.exp(scores - top)
                total = jnp.sum(expo, 1, keepdims=True)
                sums = jnp.dot(
                    expo.astype(jnp.bfloat16),
                    keys[0, :, :rank],
                    preferred_element_type=jnp.float32,
                )
                if n_chunks > 1:
                    total = state[par, :, LANES : LANES + 1] * shrink + total
                    sums = state[par, :, 2 * LANES :] * shrink + sums
                    state[par, :, :LANES] = jnp.broadcast_to(top, (pairs * span_len, LANES))
                    state[par, :, LANES : 2 * LANES] = jnp.broadcast_to(
                        total, (pairs * span_len, LANES)
                    )
                    state[par, :, 2 * LANES :] = sums
                else:
                    finish(par, sums, total)

        def finish(par, sums, total, span=span):
            result = (sums / total).astype(jnp.bfloat16)
            mixed[par, :, pl.ds(span * span_len, span_len), :] = result.reshape(
                pairs, span_len, rank
            )

        if n_chunks == 1:
            one_chunk(0)
        else:
            state[:, :, :LANES] = jnp.full((2, pairs * span_len, LANES), -1e30, jnp.float32)
            state[:, :, LANES:] = jnp.zeros((2, pairs * span_len, LANES + rank), jnp.float32)

            @pl.loop(0, n_chunks)
            def _(c):
                one_chunk(c)

            for par in range(2):
                finish(par, state[par, :, 2 * LANES :], state[par, :, LANES : LANES + 1])

    v_dim = w_ref.shape[2]
    for head in range(heads):
        out_ref[:, pl.ds(head * v_dim, v_dim)] = jnp.dot(
            mixed[head % 2, head // 2], w_ref[head], preferred_element_type=jnp.float32
        ).astype(jnp.bfloat16)


def per_device(n_seq, n_head, span_order, queries, latent_kv, w_uv):
    tok_dev = queries.shape[0]
    heads, rank, v_dim = w_uv.shape
    kv_count, width = latent_kv.shape
    span_len = tok_dev // 2
    spans = span_order.shape[0]
    spans_seq = spans // SEQS
    seq_len = spans_seq * span_len
    pairs = heads // 2
    wide = rank + LANES
    chunk_spans = min(CHUNK_SPANS, spans_seq)
    state_rows = pairs * span_len if spans_seq > chunk_spans else 8
    dims = (n_seq, n_head, heads, rank, span_len, kv_count, spans_seq)
    table = jnp.asarray(angle_table(seq_len, ROPE_DIM // 2))
    dma = pltpu.SemaphoreType.DMA
    smem = pl.BlockSpec(memory_space=pltpu.SMEM)
    vmem = pl.BlockSpec(memory_space=pltpu.VMEM)
    kv = pl.pallas_call(
        functools.partial(gather_kernel, dims),
        out_shape=jax.ShapeDtypeStruct((n_seq * n_head, kv_count, width), jnp.bfloat16),
        in_specs=[vmem],
        out_specs=vmem,
        scratch_shapes=[
            dma((max(n_head - 1, 1),)),
            dma((max(n_head - 1, 1),)),
            dma((n_head, n_seq // 2)),
            dma((n_head, n_seq // 2)),
            dma((n_head, n_seq // 2)),
            dma((n_head, n_seq // 2)),
            pltpu.SemaphoreType.REGULAR((n_head + n_seq // 2 - 1,)),
        ],
        compiler_params=pltpu.CompilerParams(
            collective_id=0, has_side_effects=True, vmem_limit_bytes=GATHER_MIB << 20
        ),
        cost_estimate=pl.CostEstimate(flops=20 << 30, bytes_accessed=1 << 20, transcendentals=0),
        name="gather_keys",
    )(latent_kv)
    return pl.pallas_call(
        functools.partial(attend_kernel, dims),
        out_shape=jax.ShapeDtypeStruct((tok_dev, heads * v_dim), jnp.bfloat16),
        in_specs=[smem, vmem, vmem, vmem, vmem],
        out_specs=vmem,
        scratch_shapes=[
            pltpu.VMEM((2, 2, pairs * span_len, wide), jnp.bfloat16),
            pltpu.VMEM((2, chunk_spans * span_len, wide), jnp.bfloat16),
            pltpu.VMEM((2, pairs, tok_dev, rank), jnp.bfloat16),
            pltpu.VMEM((2, state_rows, 2 * LANES + rank), jnp.float32),
        ],
        compiler_params=pltpu.CompilerParams(vmem_limit_bytes=ATTEND_MIB << 20),
        cost_estimate=pl.CostEstimate(flops=4 << 30, bytes_accessed=8 << 20, transcendentals=1 << 20),
        name="attend",
    )(span_order, queries, kv, table, w_uv)


def solution(mesh):
    in_specs = (P(), P("seq", "head"), P(("seq", "head"), None), P("head", None, None))
    return jax.shard_map(
        functools.partial(per_device, mesh.shape["seq"], mesh.shape["head"]),
        mesh=mesh,
        in_specs=in_specs,
        out_specs=P("seq", "head"),
        check_vma=False,
    )
```

```python
import functools
import math

import jax
import jax.numpy as jnp
import numpy as np
from jax import lax
from jax.experimental import pallas as pl
from jax.experimental.pallas import tpu as pltpu
from jax.sharding import PartitionSpec as P

ROPE_DIM = 64
NOPE_DIM = 128
SEQS = 2
LANES = 128
CHUNK_SPANS = 8
PARTS = 1
PUTS = 4
GATHER_MIB = 24
ATTEND_MIB = 40

theta_base = 10000.0
logit_scale = (NOPE_DIM + ROPE_DIM) ** -0.5
exponent_scale = logit_scale * math.log2(math.e)


def angle_table(count, half):
    freq = np.exp(-math.log(theta_base) * np.arange(half, dtype=np.float32) / half).astype(
        np.float32
    )
    phases = (np.arange(count, dtype=np.float32)[:, None] * freq[None, :]).astype(np.float64)
    cosine, sine = np.cos(phases), np.sin(phases)
    return np.concatenate([cosine, cosine, -sine, sine], 1).astype(np.float32)


def flip(index, bits):
    out = index
    place = 1
    while place <= bits:
        if bits & place:
            out = out + place * (1 - 2 * ((index // place) % 2))
        place *= 2
    return out


def rotate_tile(tile, table, high):
    lane = lax.broadcasted_iota(jnp.int32, tile.shape, tile.ndim - 1)
    quarter = lane // (ROPE_DIM // 2)
    last = tile.ndim - 1
    forward = pltpu.roll(tile, ROPE_DIM // 2, last)
    backward = pltpu.roll(tile, LANES - ROPE_DIM // 2, last)
    swapped = jnp.where(quarter % 2 == 0, backward, forward)
    turned = pltpu.roll(table, ROPE_DIM, 1)
    cosine, sine = (turned, table) if high else (table, turned)
    here = (quarter >= 2) if high else (quarter < 2)
    return jnp.where(here, tile * cosine + swapped * sine, tile)


def span_places(order_ref, s, spans_seq, span_len):
    seq_first, place = [], []
    for span in range(2):
        mine = order_ref[2 * s + span]
        first = jnp.int32(0)
        for later in range(1, SEQS):
            first = jnp.where(mine >= later * spans_seq, later * spans_seq, first)
        seq_first.append(first)
        place.append((mine - first) * span_len)
    return seq_first, place


def gather_kernel(
    dims,
    latent_ref,
    kv,
    z_send,
    z_recv,
    p_send,
    p_recv,
    d_send,
    d_recv,
    ready,
):
    n_seq, n_head, heads, rank, span_len, kv_count, spans_seq = dims
    s = lax.axis_index("seq")
    h = lax.axis_index("head")
    far = range(2, n_seq, 2)
    mesh_id = pl.DeviceIdType.MESH
    barrier = pltpu.get_barrier_semaphore()
    peers = [(d, 0) for d in far] + [(0, k) for k in range(1, n_head)] + [(1, 0)]
    peers.sort(key=lambda peer: bin(peer[0]).count("1") + (peer[1] + peer[1] // 2) * 0.9)

    def signal(sem, d, k):
        pl.semaphore_signal(
            sem,
            inc=1,
            device_id={"seq": flip(s, d), "head": flip(h, k)},
            device_id_type=mesh_id,
        )

    def later(d, k):
        return flip(h, k) > h if k else flip(s, d) > s

    sent = []

    def describe(d, k, send, recv, to_d, to_k):
        block = kv.at[flip(s, d) * n_head + flip(h, k)]
        copy = pltpu.make_async_remote_copy(
            src_ref=block if d or k else latent_ref,
            dst_ref=block,
            send_sem=send,
            recv_sem=recv,
            device_id={"seq": flip(s, to_d), "head": flip(h, to_k)},
            device_id_type=mesh_id,
        )
        sent.append(copy)
        return copy

    def arrived(d, k, send, recv):
        block = kv.at[flip(s, d) * n_head + flip(h, k)]
        pltpu.make_async_remote_copy(
            src_ref=block,
            dst_ref=block,
            send_sem=send,
            recv_sem=recv,
            device_id={"seq": flip(s, 1), "head": h},
            device_id_type=mesh_id,
        ).wait_recv()

    before = jnp.int32(0)
    for peer in peers:
        before = before + jnp.where(later(*peer), 0, 1)

        @pl.when(later(*peer))
        def _(peer=peer):
            signal(barrier, *peer)

    kv[s * n_head + h] = latent_ref[...]

    @pl.when(before > 0)
    def _():
        pl.semaphore_wait(barrier, before)

    for i, peer in enumerate(peers):

        @pl.when(jnp.logical_not(later(*peer)))
        def _(i=i, peer=peer):
            signal(ready.at[i], *peer)

    first = []
    for d, k in peers:
        if k:
            first.append(describe(0, 0, z_send.at[k - 1], z_recv.at[k - 1], 0, k))
        elif d > 1:
            first.append(describe(0, 0, p_send.at[0, d // 2], p_recv.at[0, d // 2], d, 0))
        else:
            first.append(describe(0, 0, d_send.at[0, 0], d_recv.at[0, 0], 1, 0))
    for peer, copy in zip(peers, first):
        pl.when(jnp.logical_not(later(*peer)))(copy.start)
    for i, (peer, copy) in enumerate(zip(peers, first)):

        @pl.when(later(*peer))
        def _(i=i, copy=copy):
            pl.semaphore_wait(ready.at[i], 1)
            copy.start()

    def spread(k, d):
        if d == 0:
            for to in reversed(far):
                describe(0, k, p_send.at[k, to // 2], p_recv.at[k, to // 2], to, 0).start()
        describe(d, k, d_send.at[k, d // 2], d_recv.at[k, d // 2], 1, 0).start()

    events = []
    for k in range(n_head):
        for d in range(0, n_seq, 2):
            if d:
                events.append((k + bin(d).count("1") + 2, d, k))
            elif k:
                events.append((k, d, k))
    for _, d, k in sorted(events):
        if d:
            arrived(d, k, p_send.at[k, d // 2], p_recv.at[k, d // 2])
        else:
            arrived(0, k, z_send.at[k - 1], z_recv.at[k - 1])
        spread(k, d)
    for k in range(n_head):
        for d in range(0, n_seq, 2):
            arrived(d + 1, k, d_send.at[k, d // 2], d_recv.at[k, d // 2])
    for copy in sent:
        copy.wait_send()


def attend_kernel(
    dims, order_hbm, queries_ref, kv, table, w_ref, out_ref, q_rows, keys, mixed, state, result, put_sem, order_ref, order_sem
):
    n_seq, n_head, heads, rank, span_len, kv_count, spans_seq = dims
    width = rank + ROPE_DIM
    pairs = heads // 2
    s = lax.axis_index("seq")
    spans = SEQS * spans_seq
    per_span = span_len // kv_count
    rows_all = heads * span_len
    order = pltpu.make_async_copy(order_hbm, order_ref, order_sem)
    order.start()

    def copy_queries(span):
        for par in range(2):
            for pair in range(pairs):
                source = pl.ds(span * span_len, span_len)
                first = pair * 2 * width + par * rank
                rows = pl.ds((pair * 2 + par) * span_len, span_len)
                whole = queries_ref[source, pl.ds(first, rank + LANES)]
                if par:
                    whole = pltpu.roll(whole, rank + LANES - ROPE_DIM, 1)
                q_rows[span, rows, :] = whole

    def rotate_queries(span):
        angles = table[pl.ds(place[span], span_len), :]
        for head in range(heads):
            rows = pl.ds(head * span_len, span_len)
            tail = q_rows[span, rows, rank:].astype(jnp.float32)
            q_rows[span, rows, rank:] = rotate_tile(tail, angles, False).astype(jnp.bfloat16)

    def block_of(stream_span):
        def pick(slot, found):
            return jnp.where(order_ref[slot] == stream_span, slot * per_span, found)

        if spans > 16:
            return lax.fori_loop(0, spans, pick, jnp.int32(0))
        found = jnp.int32(0)
        for slot in range(spans):
            found = pick(slot, found)
        return found

    chunk_spans = min(CHUNK_SPANS, spans_seq)
    n_chunks = spans_seq // chunk_spans
    chunk = chunk_spans * span_len

    def prepare_keys(span, c):
        for j in range(chunk_spans):
            block = block_of(seq_first[span] + c * chunk_spans + j)
            raw = kv[pl.ds(block, per_span)].reshape(span_len, width)
            angles = table[pl.ds((c * chunk_spans + j) * span_len, span_len), :]
            pad = jnp.zeros((span_len, LANES - ROPE_DIM), jnp.float32)
            rope = jnp.concatenate([raw[:, rank:].astype(jnp.float32), pad], 1)
            rows = pl.ds(j * span_len, span_len)
            keys[span, rows, :rank] = raw[:, :rank]
            keys[span, rows, rank:] = rotate_tile(rope, angles, False).astype(jnp.bfloat16)

    def one_chunk(span, c):
        limit = lax.broadcasted_iota(jnp.int32, (span_len, chunk), 0) + place[span]
        seen = lax.broadcasted_iota(jnp.int32, (span_len, chunk), 1) + c * chunk <= limit
        for part in range(PARTS):
            share = heads // PARTS
            rows = pl.ds(part * share * span_len, share * span_len)
            scores = (
                lax.dot_general(
                    q_rows[span, rows, :],
                    keys[span],
                    (((1,), (1,)), ((), ())),
                    preferred_element_type=jnp.float32,
                )
                * exponent_scale
            )
            scores = jnp.where(
                seen[None], scores.reshape(share, span_len, chunk), -jnp.inf
            ).reshape(share * span_len, chunk)
            top = jnp.max(scores, 1, keepdims=True)
            if n_chunks > 1:
                old_top = state[rows, 0:1]
                top = jnp.maximum(top, old_top)
                shrink = jnp.exp2(old_top - top)
            expo = jnp.exp2(scores - top)
            total = jnp.sum(expo, 1, keepdims=True)
            sums = jnp.dot(
                expo.astype(jnp.bfloat16),
                keys[span, :, :rank],
                preferred_element_type=jnp.float32,
            )
            if n_chunks > 1:
                total = state[rows, LANES : LANES + 1] * shrink + total
                sums = state[rows, 2 * LANES :] * shrink + sums
                state[rows, :LANES] = jnp.broadcast_to(top, (share * span_len, LANES))
                state[rows, LANES : 2 * LANES] = jnp.broadcast_to(total, (share * span_len, LANES))
                state[rows, 2 * LANES :] = sums
            else:
                finish(span, part * share, share, sums, total)

    def finish(span, first, count, sums, total):
        result = (sums * (1.0 / total)).astype(jnp.bfloat16)
        mixed[pl.ds(first, count), pl.ds(span * span_len, span_len), :] = result.reshape(
            count, span_len, rank
        )

    for span in range(2):
        copy_queries(span)
    order.wait()
    seq_first, place = span_places(order_ref, s, spans_seq, span_len)
    for span in range(2):
        rotate_queries(span)
        if n_chunks == 1:
            prepare_keys(span, 0)
            one_chunk(span, 0)
        else:
            state[:, :LANES] = jnp.full((rows_all, LANES), -1e30, jnp.float32)
            state[:, LANES:] = jnp.zeros((rows_all, LANES + rank), jnp.float32)

            @pl.loop(0, n_chunks)
            def _(c, span=span):
                prepare_keys(span, c)
                one_chunk(span, c)

            finish(span, 0, heads, state[:, 2 * LANES :], state[:, LANES : LANES + 1])

    v_dim = w_ref.shape[2]
    puts = []
    for part in range(PUTS):
        share = heads // PUTS
        for head in range(part * share, part * share + share):
            result[:, pl.ds(head * v_dim, v_dim)] = jnp.dot(
                mixed[head], w_ref[head], preferred_element_type=jnp.float32
            ).astype(jnp.bfloat16)
        lanes = pl.ds(part * share * v_dim, share * v_dim)
        puts.append(pltpu.make_async_copy(result.at[:, lanes], out_ref.at[:, lanes], put_sem.at[part]))
        puts[-1].start()
    for put in puts:
        put.wait()


def per_device(n_seq, n_head, span_order, queries, latent_kv, w_uv):
    tok_dev = queries.shape[0]
    heads, rank, v_dim = w_uv.shape
    kv_count, width = latent_kv.shape
    span_len = tok_dev // 2
    spans = span_order.shape[0]
    spans_seq = spans // SEQS
    seq_len = spans_seq * span_len
    wide = rank + LANES
    chunk_spans = min(CHUNK_SPANS, spans_seq)
    state_rows = heads * span_len if spans_seq > chunk_spans else 8
    dims = (n_seq, n_head, heads, rank, span_len, kv_count, spans_seq)
    table = jnp.asarray(angle_table(seq_len, ROPE_DIM // 2))
    dma = pltpu.SemaphoreType.DMA
    vmem = pl.BlockSpec(memory_space=pltpu.VMEM)
    kv = pl.pallas_call(
        functools.partial(gather_kernel, dims),
        out_shape=jax.ShapeDtypeStruct((n_seq * n_head, kv_count, width), jnp.bfloat16),
        in_specs=[vmem],
        out_specs=vmem,
        scratch_shapes=[
            dma((max(n_head - 1, 1),)),
            dma((max(n_head - 1, 1),)),
            dma((n_head, n_seq // 2)),
            dma((n_head, n_seq // 2)),
            dma((n_head, n_seq // 2)),
            dma((n_head, n_seq // 2)),
            pltpu.SemaphoreType.REGULAR((n_head + n_seq // 2 - 1,)),
        ],
        compiler_params=pltpu.CompilerParams(
            collective_id=0, has_side_effects=True, vmem_limit_bytes=GATHER_MIB << 20
        ),
        cost_estimate=pl.CostEstimate(flops=20 << 30, bytes_accessed=1 << 20, transcendentals=0),
        name="gather_keys",
    )(latent_kv)
    return pl.pallas_call(
        functools.partial(attend_kernel, dims),
        out_shape=jax.ShapeDtypeStruct((tok_dev, heads * v_dim), jnp.bfloat16),
        in_specs=[pl.BlockSpec(memory_space=pl.ANY), vmem, vmem, vmem, vmem],
        out_specs=pl.BlockSpec(memory_space=pl.ANY),
        scratch_shapes=[
            pltpu.VMEM((2, heads * span_len, wide), jnp.bfloat16),
            pltpu.VMEM((2, chunk_spans * span_len, wide), jnp.bfloat16),
            pltpu.VMEM((heads, tok_dev, rank), jnp.bfloat16),
            pltpu.VMEM((state_rows, 2 * LANES + rank), jnp.float32),
            pltpu.VMEM((tok_dev, heads * v_dim), jnp.bfloat16),
            dma((PUTS,)),
            pltpu.SMEM(span_order.shape, jnp.int32),
            dma,
        ],
        compiler_params=pltpu.CompilerParams(vmem_limit_bytes=ATTEND_MIB << 20),
        cost_estimate=pl.CostEstimate(flops=4 << 30, bytes_accessed=8 << 20, transcendentals=1 << 20),
        name="attend",
    )(span_order, queries, kv, table, w_uv)


def solution(mesh):
    in_specs = (P(), P("seq", "head"), P(("seq", "head"), None), P("head", None, None))
    return jax.shard_map(
        functools.partial(per_device, mesh.shape["seq"], mesh.shape["head"]),
        mesh=mesh,
        in_specs=in_specs,
        out_specs=P("seq", "head"),
        check_vma=False,
    )
```

```python
import functools
import math

import jax
import jax.numpy as jnp
import numpy as np
from jax import lax
from jax.experimental import pallas as pl
from jax.experimental.pallas import tpu as pltpu
from jax.sharding import PartitionSpec as P

ROPE_DIM = 64
NOPE_DIM = 128
SEQS = 2
LANES = 128
CHUNK_SPANS = 8
PARTS = 1
PUTS = 4
GATHER_MIB = 24
ATTEND_MIB = 40

theta_base = 10000.0
logit_scale = (NOPE_DIM + ROPE_DIM) ** -0.5
exponent_scale = logit_scale * math.log2(math.e)


def angle_table(count, half):
    freq = np.exp(-math.log(theta_base) * np.arange(half, dtype=np.float32) / half).astype(
        np.float32
    )
    phases = (np.arange(count, dtype=np.float32)[:, None] * freq[None, :]).astype(np.float64)
    cosine, sine = np.cos(phases), np.sin(phases)
    return np.concatenate([cosine, cosine, -sine, sine], 1).astype(np.float32)


def flip(index, bits):
    out = index
    place = 1
    while place <= bits:
        if bits & place:
            out = out + place * (1 - 2 * ((index // place) % 2))
        place *= 2
    return out


def rotate_tile(tile, table, high):
    lane = lax.broadcasted_iota(jnp.int32, tile.shape, tile.ndim - 1)
    quarter = lane // (ROPE_DIM // 2)
    last = tile.ndim - 1
    forward = pltpu.roll(tile, ROPE_DIM // 2, last)
    backward = pltpu.roll(tile, LANES - ROPE_DIM // 2, last)
    swapped = jnp.where(quarter % 2 == 0, backward, forward)
    turned = pltpu.roll(table, ROPE_DIM, 1)
    cosine, sine = (turned, table) if high else (table, turned)
    here = (quarter >= 2) if high else (quarter < 2)
    return jnp.where(here, tile * cosine + swapped * sine, tile)


def span_places(order_ref, s, spans_seq, span_len):
    seq_first, place = [], []
    for span in range(2):
        mine = order_ref[2 * s + span]
        first = jnp.int32(0)
        for later in range(1, SEQS):
            first = jnp.where(mine >= later * spans_seq, later * spans_seq, first)
        seq_first.append(first)
        place.append((mine - first) * span_len)
    return seq_first, place


def gather_kernel(
    dims,
    latent_ref,
    kv,
    z_send,
    z_recv,
    p_send,
    p_recv,
    d_send,
    d_recv,
    ready,
):
    n_seq, n_head, heads, rank, span_len, kv_count, spans_seq = dims
    s = lax.axis_index("seq")
    h = lax.axis_index("head")
    far = range(2, n_seq, 2)
    mesh_id = pl.DeviceIdType.MESH
    barrier = pltpu.get_barrier_semaphore()
    peers = [(d, 0) for d in far] + [(0, k) for k in range(1, n_head)] + [(1, 0)]
    peers.sort(key=lambda peer: bin(peer[0]).count("1") + (peer[1] + peer[1] // 2) * 0.9)

    def signal(sem, d, k):
        pl.semaphore_signal(
            sem,
            inc=1,
            device_id={"seq": flip(s, d), "head": flip(h, k)},
            device_id_type=mesh_id,
        )

    def later(d, k):
        return flip(h, k) > h if k else flip(s, d) > s

    sent = []

    def describe(d, k, send, recv, to_d, to_k):
        block = kv.at[flip(s, d) * n_head + flip(h, k)]
        copy = pltpu.make_async_remote_copy(
            src_ref=block,
            dst_ref=block,
            send_sem=send,
            recv_sem=recv,
            device_id={"seq": flip(s, to_d), "head": flip(h, to_k)},
            device_id_type=mesh_id,
        )
        sent.append(copy)
        return copy

    def arrived(d, k, send, recv):
        block = kv.at[flip(s, d) * n_head + flip(h, k)]
        pltpu.make_async_remote_copy(
            src_ref=block,
            dst_ref=block,
            send_sem=send,
            recv_sem=recv,
            device_id={"seq": flip(s, 1), "head": h},
            device_id_type=mesh_id,
        ).wait_recv()

    mine = s * n_head + h
    for c in range(0, rank, LANES):
        kv[mine, pl.ds(c // LANES * kv_count, kv_count), :] = latent_ref[:, pl.ds(c, LANES)]
    tail = latent_ref[:, rank:].astype(jnp.float32)
    tail = jnp.concatenate([tail, jnp.zeros((kv_count, LANES - ROPE_DIM), jnp.float32)], 1)
    low, high = tail[: kv_count // 2], tail[kv_count // 2 :]
    kv[mine, pl.ds(rank // LANES * kv_count, kv_count // 2), :] = (
        low + pltpu.roll(high, ROPE_DIM, 1)
    ).astype(jnp.bfloat16)

    before = jnp.int32(0)
    for peer in peers:
        before = before + jnp.where(later(*peer), 0, 1)

        @pl.when(later(*peer))
        def _(peer=peer):
            signal(barrier, *peer)


    @pl.when(before > 0)
    def _():
        pl.semaphore_wait(barrier, before)

    for i, peer in enumerate(peers):

        @pl.when(jnp.logical_not(later(*peer)))
        def _(i=i, peer=peer):
            signal(ready.at[i], *peer)

    first = []
    for d, k in peers:
        if k:
            first.append(describe(0, 0, z_send.at[k - 1], z_recv.at[k - 1], 0, k))
        elif d > 1:
            first.append(describe(0, 0, p_send.at[0, d // 2], p_recv.at[0, d // 2], d, 0))
        else:
            first.append(describe(0, 0, d_send.at[0, 0], d_recv.at[0, 0], 1, 0))
    for peer, copy in zip(peers, first):
        near = flip(h, peer[1]) != 0
        pl.when(jnp.logical_not(later(*peer)) & jnp.logical_not(near))(copy.start)
    for peer, copy in zip(peers, first):
        near = flip(h, peer[1]) != 0
        pl.when(jnp.logical_not(later(*peer)) & near)(copy.start)
    def send_later(chosen):
        for i, (peer, copy) in enumerate(zip(peers, first)):
            distant = flip(h, peer[1]) - h >= n_head - 1
            if peer[1]:
                due = later(*peer) & (distant == chosen)
            elif chosen:
                continue
            else:
                due = later(*peer)

            @pl.when(due)
            def _(i=i, copy=copy):
                pl.semaphore_wait(ready.at[i], 1)
                copy.start()

    send_later(False)

    def spread(k, d):
        if d == 0:
            for to in reversed(far):
                describe(0, k, p_send.at[k, to // 2], p_recv.at[k, to // 2], to, 0).start()
        describe(d, k, d_send.at[k, d // 2], d_recv.at[k, d // 2], 1, 0).start()

    events = []
    for k in range(n_head):
        for d in range(0, n_seq, 2):
            if d:
                events.append((k + 3 + (bin(d).count("1") - 1) * 0.05, d, k))
            elif k:
                events.append((k, d, k))
    for turn, (_, d, k) in enumerate(sorted(events)):
        if turn == 1:
            send_later(True)
        if d:
            arrived(d, k, p_send.at[k, d // 2], p_recv.at[k, d // 2])
        else:
            arrived(0, k, z_send.at[k - 1], z_recv.at[k - 1])
        spread(k, d)
    for k in range(n_head):
        for d in range(0, n_seq, 2):
            arrived(d + 1, k, d_send.at[k, d // 2], d_recv.at[k, d // 2])
    for copy in sent:
        copy.wait_send()


def attend_kernel(
    dims, order_hbm, queries_ref, kv, table, w_ref, out_ref, q_rows, keys, mixed, state, result, put_sem, order_ref, order_sem
):
    n_seq, n_head, heads, rank, span_len, kv_count, spans_seq = dims
    width = rank + ROPE_DIM
    pairs = heads // 2
    s = lax.axis_index("seq")
    spans = SEQS * spans_seq
    per_span = span_len // kv_count
    rows_all = heads * span_len
    order = pltpu.make_async_copy(order_hbm, order_ref, order_sem)
    order.start()

    def copy_queries(span):
        for par in range(2):
            for pair in range(pairs):
                source = pl.ds(span * span_len, span_len)
                first = pair * 2 * width + par * rank
                rows = pl.ds((pair * 2 + par) * span_len, span_len)
                whole = queries_ref[source, pl.ds(first, rank + LANES)]
                if par:
                    whole = pltpu.roll(whole, rank + LANES - ROPE_DIM, 1)
                q_rows[span, rows, :] = whole

    def rotate_queries(span):
        angles = table[pl.ds(place[span], span_len), :]
        for head in range(heads):
            rows = pl.ds(head * span_len, span_len)
            tail = q_rows[span, rows, rank:].astype(jnp.float32)
            q_rows[span, rows, rank:] = rotate_tile(tail, angles, False).astype(jnp.bfloat16)

    def block_of(stream_span):
        def pick(slot, found):
            return jnp.where(order_ref[slot] == stream_span, slot * per_span, found)

        if spans > 16:
            return lax.fori_loop(0, spans, pick, jnp.int32(0))
        found = jnp.int32(0)
        for slot in range(spans):
            found = pick(slot, found)
        return found

    chunk_spans = min(CHUNK_SPANS, spans_seq)
    n_chunks = spans_seq // chunk_spans
    chunk = chunk_spans * span_len

    def prepare_keys(span, c):
        for j in range(chunk_spans):
            block = block_of(seq_first[span] + c * chunk_spans + j)
            angles = table[pl.ds((c * chunk_spans + j) * span_len, span_len), :]
            rope = []
            for piece in range(per_span):
                rows = pl.ds(j * span_len + piece * kv_count, kv_count)
                for t in range(rank // LANES):
                    keys[span, rows, pl.ds(t * LANES, LANES)] = kv[
                        block + piece, pl.ds(t * kv_count, kv_count), :
                    ]
                tail = kv[block + piece, pl.ds(rank // LANES * kv_count, kv_count // 2), :]
                tail = tail.astype(jnp.float32)
                rope += [tail, pltpu.roll(tail, LANES - ROPE_DIM, 1)]
            rope = rotate_tile(jnp.concatenate(rope, 0), angles, False)
            lane = lax.broadcasted_iota(jnp.int32, rope.shape, 1)
            rows = pl.ds(j * span_len, span_len)
            keys[span, rows, rank:] = jnp.where(lane < ROPE_DIM, rope, 0.0).astype(jnp.bfloat16)

    def one_chunk(span, c):
        limit = lax.broadcasted_iota(jnp.int32, (span_len, chunk), 0) + place[span]
        seen = lax.broadcasted_iota(jnp.int32, (span_len, chunk), 1) + c * chunk <= limit
        for part in range(PARTS):
            share = heads // PARTS
            rows = pl.ds(part * share * span_len, share * span_len)
            scores = (
                lax.dot_general(
                    q_rows[span, rows, :],
                    keys[span],
                    (((1,), (1,)), ((), ())),
                    preferred_element_type=jnp.float32,
                )
                * exponent_scale
            )
            scores = jnp.where(
                seen[None], scores.reshape(share, span_len, chunk), -jnp.inf
            ).reshape(share * span_len, chunk)
            top = jnp.max(scores, 1, keepdims=True)
            if n_chunks > 1:
                old_top = state[rows, 0:1]
                top = jnp.maximum(top, old_top)
                shrink = jnp.exp2(old_top - top)
            expo = jnp.exp2(scores - top)
            total = jnp.sum(expo, 1, keepdims=True)
            sums = jnp.dot(
                expo.astype(jnp.bfloat16),
                keys[span, :, :rank],
                preferred_element_type=jnp.float32,
            )
            if n_chunks > 1:
                total = state[rows, LANES : LANES + 1] * shrink + total
                sums = state[rows, 2 * LANES :] * shrink + sums
                state[rows, :LANES] = jnp.broadcast_to(top, (share * span_len, LANES))
                state[rows, LANES : 2 * LANES] = jnp.broadcast_to(total, (share * span_len, LANES))
                state[rows, 2 * LANES :] = sums
            else:
                finish(span, part * share, share, sums, total)

    def finish(span, first, count, sums, total):
        result = (sums * (1.0 / total)).astype(jnp.bfloat16)
        mixed[pl.ds(first, count), pl.ds(span * span_len, span_len), :] = result.reshape(
            count, span_len, rank
        )

    for span in range(2):
        copy_queries(span)
    order.wait()
    seq_first, place = span_places(order_ref, s, spans_seq, span_len)
    for span in range(2):
        rotate_queries(span)
        if n_chunks == 1:
            prepare_keys(span, 0)
            one_chunk(span, 0)
        else:
            state[:, :LANES] = jnp.full((rows_all, LANES), -1e30, jnp.float32)
            state[:, LANES:] = jnp.zeros((rows_all, LANES + rank), jnp.float32)

            @pl.loop(0, n_chunks)
            def _(c, span=span):
                prepare_keys(span, c)
                one_chunk(span, c)

            finish(span, 0, heads, state[:, 2 * LANES :], state[:, LANES : LANES + 1])

    v_dim = w_ref.shape[2]
    puts = []
    for part in range(PUTS):
        share = heads // PUTS
        for head in range(part * share, part * share + share):
            result[:, pl.ds(head * v_dim, v_dim)] = jnp.dot(
                mixed[head], w_ref[head], preferred_element_type=jnp.float32
            ).astype(jnp.bfloat16)
        lanes = pl.ds(part * share * v_dim, share * v_dim)
        puts.append(pltpu.make_async_copy(result.at[:, lanes], out_ref.at[:, lanes], put_sem.at[part]))
        puts[-1].start()
    for put in puts:
        put.wait()


def per_device(n_seq, n_head, span_order, queries, latent_kv, w_uv):
    tok_dev = queries.shape[0]
    heads, rank, v_dim = w_uv.shape
    kv_count, width = latent_kv.shape
    span_len = tok_dev // 2
    spans = span_order.shape[0]
    spans_seq = spans // SEQS
    seq_len = spans_seq * span_len
    wide = rank + LANES
    packed = kv_count * width // LANES
    chunk_spans = min(CHUNK_SPANS, spans_seq)
    state_rows = heads * span_len if spans_seq > chunk_spans else 8
    dims = (n_seq, n_head, heads, rank, span_len, kv_count, spans_seq)
    table = jnp.asarray(angle_table(seq_len, ROPE_DIM // 2))
    dma = pltpu.SemaphoreType.DMA
    vmem = pl.BlockSpec(memory_space=pltpu.VMEM)
    kv = pl.pallas_call(
        functools.partial(gather_kernel, dims),
        out_shape=jax.ShapeDtypeStruct((n_seq * n_head, packed, LANES), jnp.bfloat16),
        in_specs=[vmem],
        out_specs=vmem,
        scratch_shapes=[
            dma((max(n_head - 1, 1),)),
            dma((max(n_head - 1, 1),)),
            dma((n_head, n_seq // 2)),
            dma((n_head, n_seq // 2)),
            dma((n_head, n_seq // 2)),
            dma((n_head, n_seq // 2)),
            pltpu.SemaphoreType.REGULAR((n_head + n_seq // 2 - 1,)),
        ],
        compiler_params=pltpu.CompilerParams(
            collective_id=0, has_side_effects=True, vmem_limit_bytes=GATHER_MIB << 20
        ),
        cost_estimate=pl.CostEstimate(flops=20 << 30, bytes_accessed=1 << 20, transcendentals=0),
        name="gather_keys",
    )(latent_kv)
    return pl.pallas_call(
        functools.partial(attend_kernel, dims),
        out_shape=jax.ShapeDtypeStruct((tok_dev, heads * v_dim), jnp.bfloat16),
        in_specs=[pl.BlockSpec(memory_space=pl.ANY), vmem, vmem, vmem, vmem],
        out_specs=pl.BlockSpec(memory_space=pl.ANY),
        scratch_shapes=[
            pltpu.VMEM((2, heads * span_len, wide), jnp.bfloat16),
            pltpu.VMEM((2, chunk_spans * span_len, wide), jnp.bfloat16),
            pltpu.VMEM((heads, tok_dev, rank), jnp.bfloat16),
            pltpu.VMEM((state_rows, 2 * LANES + rank), jnp.float32),
            pltpu.VMEM((tok_dev, heads * v_dim), jnp.bfloat16),
            dma((PUTS,)),
            pltpu.SMEM(span_order.shape, jnp.int32),
            dma,
        ],
        compiler_params=pltpu.CompilerParams(vmem_limit_bytes=ATTEND_MIB << 20),
        cost_estimate=pl.CostEstimate(flops=4 << 30, bytes_accessed=8 << 20, transcendentals=1 << 20),
        name="attend",
    )(span_order, queries, kv, table, w_uv)


def solution(mesh):
    in_specs = (P(), P("seq", "head"), P(("seq", "head"), None), P("head", None, None))
    return jax.shard_map(
        functools.partial(per_device, mesh.shape["seq"], mesh.shape["head"]),
        mesh=mesh,
        in_specs=in_specs,
        out_specs=P("seq", "head"),
        check_vma=False,
    )
```

```python
import functools
import math

import jax
import jax.numpy as jnp
import numpy as np
from jax import lax
from jax.experimental import pallas as pl
from jax.experimental.pallas import tpu as pltpu
from jax.sharding import PartitionSpec as P

ROPE_DIM = 64
NOPE_DIM = 128
SEQS = 2
LANES = 128
CHUNK_SPANS = 8
PARTS = 1
PUTS = 4
GATHER_MIB = 24
ATTEND_MIB = 40

theta_base = 10000.0
logit_scale = (NOPE_DIM + ROPE_DIM) ** -0.5
exponent_scale = logit_scale * math.log2(math.e)


def angle_table(count, half):
    freq = np.exp(-math.log(theta_base) * np.arange(half, dtype=np.float32) / half).astype(
        np.float32
    )
    phases = (np.arange(count, dtype=np.float32)[:, None] * freq[None, :]).astype(np.float64)
    cosine, sine = np.cos(phases), np.sin(phases)
    return np.concatenate([cosine, cosine, -sine, sine], 1).astype(np.float32)


def flip(index, bits):
    out = index
    place = 1
    while place <= bits:
        if bits & place:
            out = out + place * (1 - 2 * ((index // place) % 2))
        place *= 2
    return out


def rotate_tile(tile, table, high):
    lane = lax.broadcasted_iota(jnp.int32, tile.shape, tile.ndim - 1)
    quarter = lane // (ROPE_DIM // 2)
    last = tile.ndim - 1
    forward = pltpu.roll(tile, ROPE_DIM // 2, last)
    backward = pltpu.roll(tile, LANES - ROPE_DIM // 2, last)
    swapped = jnp.where(quarter % 2 == 0, backward, forward)
    turned = pltpu.roll(table, ROPE_DIM, 1)
    cosine, sine = (turned, table) if high else (table, turned)
    here = (quarter >= 2) if high else (quarter < 2)
    return jnp.where(here, tile * cosine + swapped * sine, tile)


def span_places(order_ref, s, spans_seq, span_len):
    seq_first, place = [], []
    for span in range(2):
        mine = order_ref[2 * s + span]
        first = jnp.int32(0)
        for later in range(1, SEQS):
            first = jnp.where(mine >= later * spans_seq, later * spans_seq, first)
        seq_first.append(first)
        place.append((mine - first) * span_len)
    return seq_first, place


def gather_kernel(
    dims,
    latent_ref,
    kv,
    z_send,
    z_recv,
    p_send,
    p_recv,
    d_send,
    d_recv,
    ready,
):
    n_seq, n_head, heads, rank, span_len, kv_count, spans_seq = dims
    s = lax.axis_index("seq")
    h = lax.axis_index("head")
    far = range(2, n_seq, 2)
    mesh_id = pl.DeviceIdType.MESH
    barrier = pltpu.get_barrier_semaphore()
    peers = [(d, 0) for d in far] + [(0, k) for k in range(1, n_head)] + [(1, 0)]
    peers.sort(key=lambda peer: bin(peer[0]).count("1") + (peer[1] + peer[1] // 2) * 0.9)

    def signal(sem, d, k):
        pl.semaphore_signal(
            sem,
            inc=1,
            device_id={"seq": flip(s, d), "head": flip(h, k)},
            device_id_type=mesh_id,
        )

    def later(d, k):
        if d == 1:
            return s % 2 == 1
        return flip(h, k) > h if k else flip(s, d) > s

    sent = []

    def describe(d, k, send, recv, to_d, to_k):
        block = kv.at[flip(s, d) * n_head + flip(h, k)]
        copy = pltpu.make_async_remote_copy(
            src_ref=block,
            dst_ref=block,
            send_sem=send,
            recv_sem=recv,
            device_id={"seq": flip(s, to_d), "head": flip(h, to_k)},
            device_id_type=mesh_id,
        )
        sent.append(copy)
        return copy

    def arrived(d, k, send, recv):
        block = kv.at[flip(s, d) * n_head + flip(h, k)]
        pltpu.make_async_remote_copy(
            src_ref=block,
            dst_ref=block,
            send_sem=send,
            recv_sem=recv,
            device_id={"seq": flip(s, 1), "head": h},
            device_id_type=mesh_id,
        ).wait_recv()

    mine = s * n_head + h
    for c in range(0, rank, LANES):
        kv[mine, pl.ds(c // LANES * kv_count, kv_count), :] = latent_ref[:, pl.ds(c, LANES)]
    tail = latent_ref[:, rank:].astype(jnp.float32)
    tail = jnp.concatenate([tail, jnp.zeros((kv_count, LANES - ROPE_DIM), jnp.float32)], 1)
    low, high = tail[: kv_count // 2], tail[kv_count // 2 :]
    kv[mine, pl.ds(rank // LANES * kv_count, kv_count // 2), :] = (
        low + pltpu.roll(high, ROPE_DIM, 1)
    ).astype(jnp.bfloat16)

    before = jnp.int32(0)
    for peer in peers:
        before = before + jnp.where(later(*peer), 0, 1)

        @pl.when(later(*peer))
        def _(peer=peer):
            signal(barrier, *peer)


    @pl.when(before > 0)
    def _():
        pl.semaphore_wait(barrier, before)

    for i, peer in enumerate(peers):

        @pl.when(jnp.logical_not(later(*peer)))
        def _(i=i, peer=peer):
            signal(ready.at[i], *peer)

    first = []
    for d, k in peers:
        if k:
            first.append(describe(0, 0, z_send.at[k - 1], z_recv.at[k - 1], 0, k))
        elif d > 1:
            first.append(describe(0, 0, p_send.at[0, d // 2], p_recv.at[0, d // 2], d, 0))
        else:
            first.append(describe(0, 0, d_send.at[0, 0], d_recv.at[0, 0], 1, 0))
    for peer, copy in zip(peers, first):
        near = flip(h, peer[1]) != 0
        pl.when(jnp.logical_not(later(*peer)) & jnp.logical_not(near))(copy.start)
    for peer, copy in zip(peers, first):
        near = flip(h, peer[1]) != 0
        pl.when(jnp.logical_not(later(*peer)) & near)(copy.start)
    def send_later(chosen):
        for i, (peer, copy) in enumerate(zip(peers, first)):
            distant = flip(h, peer[1]) - h >= n_head - 1
            if peer[1]:
                due = later(*peer) & (distant == chosen)
            elif chosen:
                continue
            else:
                due = later(*peer)

            @pl.when(due)
            def _(i=i, copy=copy):
                pl.semaphore_wait(ready.at[i], 1)
                copy.start()

    send_later(False)

    def spread(k, d):
        if d == 0:
            for to in reversed(far):
                describe(0, k, p_send.at[k, to // 2], p_recv.at[k, to // 2], to, 0).start()
        describe(d, k, d_send.at[k, d // 2], d_recv.at[k, d // 2], 1, 0).start()

    events = []
    for k in range(n_head):
        for d in range(0, n_seq, 2):
            if d:
                events.append((k + 3 + (bin(d).count("1") - 1) * 0.05, d, k))
            elif k:
                events.append((k, d, k))
    for turn, (_, d, k) in enumerate(sorted(events)):
        if turn == 1:
            send_later(True)
        if d:
            arrived(d, k, p_send.at[k, d // 2], p_recv.at[k, d // 2])
        else:
            arrived(0, k, z_send.at[k - 1], z_recv.at[k - 1])
        spread(k, d)
    for k in range(n_head):
        for d in range(0, n_seq, 2):
            arrived(d + 1, k, d_send.at[k, d // 2], d_recv.at[k, d // 2])
    for copy in sent:
        copy.wait_send()


def attend_kernel(
    dims, order_hbm, queries_ref, kv, table, w_ref, out_ref, q_rows, keys, mixed, state, result, put_sem, order_ref, order_sem
):
    n_seq, n_head, heads, rank, span_len, kv_count, spans_seq = dims
    width = rank + ROPE_DIM
    pairs = heads // 2
    s = lax.axis_index("seq")
    spans = SEQS * spans_seq
    per_span = span_len // kv_count
    rows_all = heads * span_len
    order = pltpu.make_async_copy(order_hbm, order_ref, order_sem)
    order.start()

    def copy_queries(span):
        for par in range(2):
            for pair in range(pairs):
                source = pl.ds(span * span_len, span_len)
                first = pair * 2 * width + par * rank
                rows = pl.ds((pair * 2 + par) * span_len, span_len)
                whole = queries_ref[source, pl.ds(first, rank + LANES)]
                if par:
                    whole = pltpu.roll(whole, rank + LANES - ROPE_DIM, 1)
                q_rows[span, rows, :] = whole

    def rotate_queries(span):
        angles = table[pl.ds(place[span], span_len), :]
        for head in range(heads):
            rows = pl.ds(head * span_len, span_len)
            tail = q_rows[span, rows, rank:].astype(jnp.float32)
            q_rows[span, rows, rank:] = rotate_tile(tail, angles, False).astype(jnp.bfloat16)

    def block_of(stream_span):
        def pick(slot, found):
            return jnp.where(order_ref[slot] == stream_span, slot * per_span, found)

        if spans > 16:
            return lax.fori_loop(0, spans, pick, jnp.int32(0))
        found = jnp.int32(0)
        for slot in range(spans):
            found = pick(slot, found)
        return found

    chunk_spans = min(CHUNK_SPANS, spans_seq)
    n_chunks = spans_seq // chunk_spans
    chunk = chunk_spans * span_len

    def prepare_keys(span, c):
        for j in range(chunk_spans):
            block = block_of(seq_first[span] + c * chunk_spans + j)
            angles = table[pl.ds((c * chunk_spans + j) * span_len, span_len), :]
            rope = []
            for piece in range(per_span):
                rows = pl.ds(j * span_len + piece * kv_count, kv_count)
                for t in range(rank // LANES):
                    keys[span, rows, pl.ds(t * LANES, LANES)] = kv[
                        block + piece, pl.ds(t * kv_count, kv_count), :
                    ]
                tail = kv[block + piece, pl.ds(rank // LANES * kv_count, kv_count // 2), :]
                tail = tail.astype(jnp.float32)
                rope += [tail, pltpu.roll(tail, LANES - ROPE_DIM, 1)]
            rope = rotate_tile(jnp.concatenate(rope, 0), angles, False)
            lane = lax.broadcasted_iota(jnp.int32, rope.shape, 1)
            rows = pl.ds(j * span_len, span_len)
            keys[span, rows, rank:] = jnp.where(lane < ROPE_DIM, rope, 0.0).astype(jnp.bfloat16)

    def one_chunk(span, c):
        limit = lax.broadcasted_iota(jnp.int32, (span_len, chunk), 0) + place[span]
        seen = lax.broadcasted_iota(jnp.int32, (span_len, chunk), 1) + c * chunk <= limit
        for part in range(PARTS):
            share = heads // PARTS
            rows = pl.ds(part * share * span_len, share * span_len)
            scores = (
                lax.dot_general(
                    q_rows[span, rows, :],
                    keys[span],
                    (((1,), (1,)), ((), ())),
                    preferred_element_type=jnp.float32,
                )
                * exponent_scale
            )
            scores = jnp.where(
                seen[None], scores.reshape(share, span_len, chunk), -jnp.inf
            ).reshape(share * span_len, chunk)
            top = jnp.max(scores, 1, keepdims=True)
            if n_chunks > 1:
                old_top = state[rows, 0:1]
                top = jnp.maximum(top, old_top)
                shrink = jnp.exp2(old_top - top)
            expo = jnp.exp2(scores - top)
            total = jnp.sum(expo, 1, keepdims=True)
            sums = jnp.dot(
                expo.astype(jnp.bfloat16),
                keys[span, :, :rank],
                preferred_element_type=jnp.float32,
            )
            if n_chunks > 1:
                total = state[rows, LANES : LANES + 1] * shrink + total
                sums = state[rows, 2 * LANES :] * shrink + sums
                state[rows, :LANES] = jnp.broadcast_to(top, (share * span_len, LANES))
                state[rows, LANES : 2 * LANES] = jnp.broadcast_to(total, (share * span_len, LANES))
                state[rows, 2 * LANES :] = sums
            else:
                finish(span, part * share, share, sums, total)

    def finish(span, first, count, sums, total):
        result = (sums * (1.0 / total)).astype(jnp.bfloat16)
        mixed[pl.ds(first, count), pl.ds(span * span_len, span_len), :] = result.reshape(
            count, span_len, rank
        )

    for span in range(2):
        copy_queries(span)
    order.wait()
    seq_first, place = span_places(order_ref, s, spans_seq, span_len)
    for span in range(2):
        rotate_queries(span)
        if n_chunks == 1:
            prepare_keys(span, 0)
            one_chunk(span, 0)
        else:
            state[:, :LANES] = jnp.full((rows_all, LANES), -1e30, jnp.float32)
            state[:, LANES:] = jnp.zeros((rows_all, LANES + rank), jnp.float32)

            @pl.loop(0, n_chunks)
            def _(c, span=span):
                prepare_keys(span, c)
                one_chunk(span, c)

            finish(span, 0, heads, state[:, 2 * LANES :], state[:, LANES : LANES + 1])

    v_dim = w_ref.shape[2]
    puts = []
    for part in range(PUTS):
        share = heads // PUTS
        for head in range(part * share, part * share + share):
            result[:, pl.ds(head * v_dim, v_dim)] = jnp.dot(
                mixed[head], w_ref[head], preferred_element_type=jnp.float32
            ).astype(jnp.bfloat16)
        lanes = pl.ds(part * share * v_dim, share * v_dim)
        puts.append(pltpu.make_async_copy(result.at[:, lanes], out_ref.at[:, lanes], put_sem.at[part]))
        puts[-1].start()
    for put in puts:
        put.wait()


def per_device(n_seq, n_head, span_order, queries, latent_kv, w_uv):
    tok_dev = queries.shape[0]
    heads, rank, v_dim = w_uv.shape
    kv_count, width = latent_kv.shape
    span_len = tok_dev // 2
    spans = span_order.shape[0]
    spans_seq = spans // SEQS
    seq_len = spans_seq * span_len
    wide = rank + LANES
    packed = kv_count * width // LANES
    chunk_spans = min(CHUNK_SPANS, spans_seq)
    state_rows = heads * span_len if spans_seq > chunk_spans else 8
    dims = (n_seq, n_head, heads, rank, span_len, kv_count, spans_seq)
    table = jnp.asarray(angle_table(seq_len, ROPE_DIM // 2))
    dma = pltpu.SemaphoreType.DMA
    vmem = pl.BlockSpec(memory_space=pltpu.VMEM)
    kv = pl.pallas_call(
        functools.partial(gather_kernel, dims),
        out_shape=jax.ShapeDtypeStruct((n_seq * n_head, packed, LANES), jnp.bfloat16),
        in_specs=[vmem],
        out_specs=vmem,
        scratch_shapes=[
            dma((max(n_head - 1, 1),)),
            dma((max(n_head - 1, 1),)),
            dma((n_head, n_seq // 2)),
            dma((n_head, n_seq // 2)),
            dma((n_head, n_seq // 2)),
            dma((n_head, n_seq // 2)),
            pltpu.SemaphoreType.REGULAR((n_head + n_seq // 2 - 1,)),
        ],
        compiler_params=pltpu.CompilerParams(
            collective_id=0, has_side_effects=True, vmem_limit_bytes=GATHER_MIB << 20
        ),
        cost_estimate=pl.CostEstimate(flops=20 << 30, bytes_accessed=1 << 20, transcendentals=0),
        name="gather_keys",
    )(latent_kv)
    return pl.pallas_call(
        functools.partial(attend_kernel, dims),
        out_shape=jax.ShapeDtypeStruct((tok_dev, heads * v_dim), jnp.bfloat16),
        in_specs=[pl.BlockSpec(memory_space=pl.ANY), vmem, vmem, vmem, vmem],
        out_specs=pl.BlockSpec(memory_space=pl.ANY),
        scratch_shapes=[
            pltpu.VMEM((2, heads * span_len, wide), jnp.bfloat16),
            pltpu.VMEM((2, chunk_spans * span_len, wide), jnp.bfloat16),
            pltpu.VMEM((heads, tok_dev, rank), jnp.bfloat16),
            pltpu.VMEM((state_rows, 2 * LANES + rank), jnp.float32),
            pltpu.VMEM((tok_dev, heads * v_dim), jnp.bfloat16),
            dma((PUTS,)),
            pltpu.SMEM(span_order.shape, jnp.int32),
            dma,
        ],
        compiler_params=pltpu.CompilerParams(vmem_limit_bytes=ATTEND_MIB << 20),
        cost_estimate=pl.CostEstimate(flops=4 << 30, bytes_accessed=8 << 20, transcendentals=1 << 20),
        name="attend",
    )(span_order, queries, kv, table, w_uv)


def solution(mesh):
    in_specs = (P(), P("seq", "head"), P(("seq", "head"), None), P("head", None, None))
    return jax.shard_map(
        functools.partial(per_device, mesh.shape["seq"], mesh.shape["head"]),
        mesh=mesh,
        in_specs=in_specs,
        out_specs=P("seq", "head"),
        check_vma=False,
    )
```

```python
import functools
import math

import jax
import jax.numpy as jnp
import numpy as np
from jax import lax
from jax.experimental import pallas as pl
from jax.experimental.pallas import tpu as pltpu
from jax.sharding import PartitionSpec as P

ROPE_DIM = 64
NOPE_DIM = 128
SEQS = 2
LANES = 128
CHUNK_SPANS = 8
PARTS = 1
PUTS = 4
GATHER_MIB = 24
ATTEND_MIB = 40

theta_base = 10000.0
logit_scale = (NOPE_DIM + ROPE_DIM) ** -0.5
exponent_scale = logit_scale * math.log2(math.e)


def angle_table(count, half):
    freq = np.exp(-math.log(theta_base) * np.arange(half, dtype=np.float32) / half).astype(
        np.float32
    )
    phases = (np.arange(count, dtype=np.float32)[:, None] * freq[None, :]).astype(np.float64)
    cosine, sine = np.cos(phases), np.sin(phases)
    return np.concatenate([cosine, cosine, -sine, sine], 1).astype(np.float32)


def flip(index, bits):
    out = index
    place = 1
    while place <= bits:
        if bits & place:
            out = out + place * (1 - 2 * ((index // place) % 2))
        place *= 2
    return out


def rotate_tile(tile, table, high):
    lane = lax.broadcasted_iota(jnp.int32, tile.shape, tile.ndim - 1)
    quarter = lane // (ROPE_DIM // 2)
    last = tile.ndim - 1
    forward = pltpu.roll(tile, ROPE_DIM // 2, last)
    backward = pltpu.roll(tile, LANES - ROPE_DIM // 2, last)
    swapped = jnp.where(quarter % 2 == 0, backward, forward)
    turned = pltpu.roll(table, ROPE_DIM, 1)
    cosine, sine = (turned, table) if high else (table, turned)
    here = (quarter >= 2) if high else (quarter < 2)
    return jnp.where(here, tile * cosine + swapped * sine, tile)


def span_places(order_ref, s, spans_seq, span_len):
    seq_first, place = [], []
    for span in range(2):
        mine = order_ref[2 * s + span]
        first = jnp.int32(0)
        for later in range(1, SEQS):
            first = jnp.where(mine >= later * spans_seq, later * spans_seq, first)
        seq_first.append(first)
        place.append((mine - first) * span_len)
    return seq_first, place


def gather_kernel(
    dims,
    latent_ref,
    kv,
    z_send,
    z_recv,
    p_send,
    p_recv,
    d_send,
    d_recv,
    ready,
):
    n_seq, n_head, heads, rank, span_len, kv_count, spans_seq = dims
    s = lax.axis_index("seq")
    h = lax.axis_index("head")
    far = range(2, n_seq, 2)
    mesh_id = pl.DeviceIdType.MESH
    barrier = pltpu.get_barrier_semaphore()
    peers = [(d, 0) for d in far] + [(0, k) for k in range(1, n_head)] + [(1, 0)]
    peers.sort(
        key=lambda peer: bin(peer[0]).count("1") + (peer[1] + peer[1] // 2) * 1.05 + 0.1 * (peer[0] == 1)
    )

    def signal(sem, d, k):
        pl.semaphore_signal(
            sem,
            inc=1,
            device_id={"seq": flip(s, d), "head": flip(h, k)},
            device_id_type=mesh_id,
        )

    def later(d, k):
        if d == 1:
            return s % 2 == 1
        return flip(h, k) > h if k else flip(s, d) > s

    sent = []

    def describe(d, k, send, recv, to_d, to_k):
        block = kv.at[flip(s, d) * n_head + flip(h, k)]
        copy = pltpu.make_async_remote_copy(
            src_ref=block,
            dst_ref=block,
            send_sem=send,
            recv_sem=recv,
            device_id={"seq": flip(s, to_d), "head": flip(h, to_k)},
            device_id_type=mesh_id,
        )
        sent.append(copy)
        return copy

    def arrived(d, k, send, recv):
        block = kv.at[flip(s, d) * n_head + flip(h, k)]
        pltpu.make_async_remote_copy(
            src_ref=block,
            dst_ref=block,
            send_sem=send,
            recv_sem=recv,
            device_id={"seq": flip(s, 1), "head": h},
            device_id_type=mesh_id,
        ).wait_recv()

    mine = s * n_head + h
    for c in range(0, rank, LANES):
        kv[mine, pl.ds(c // LANES * kv_count, kv_count), :] = latent_ref[:, pl.ds(c, LANES)]
    tail = latent_ref[:, rank:].astype(jnp.float32)
    tail = jnp.concatenate([tail, jnp.zeros((kv_count, LANES - ROPE_DIM), jnp.float32)], 1)
    low, high = tail[: kv_count // 2], tail[kv_count // 2 :]
    kv[mine, pl.ds(rank // LANES * kv_count, kv_count // 2), :] = (
        low + pltpu.roll(high, ROPE_DIM, 1)
    ).astype(jnp.bfloat16)

    before = jnp.int32(0)
    for peer in peers:
        before = before + jnp.where(later(*peer), 0, 1)

        @pl.when(later(*peer))
        def _(peer=peer):
            signal(barrier, *peer)


    @pl.when(before > 0)
    def _():
        pl.semaphore_wait(barrier, before)

    for i, peer in enumerate(peers):

        @pl.when(jnp.logical_not(later(*peer)))
        def _(i=i, peer=peer):
            signal(ready.at[i], *peer)

    first = []
    for d, k in peers:
        if k:
            first.append(describe(0, 0, z_send.at[k - 1], z_recv.at[k - 1], 0, k))
        elif d > 1:
            first.append(describe(0, 0, p_send.at[0, d // 2], p_recv.at[0, d // 2], d, 0))
        else:
            first.append(describe(0, 0, d_send.at[0, 0], d_recv.at[0, 0], 1, 0))
    for peer, copy in zip(peers, first):
        near = flip(h, peer[1]) != 0
        pl.when(jnp.logical_not(later(*peer)) & jnp.logical_not(near))(copy.start)
    for peer, copy in zip(peers, first):
        near = flip(h, peer[1]) != 0
        pl.when(jnp.logical_not(later(*peer)) & near)(copy.start)
    def send_later(chosen):
        for i, (peer, copy) in enumerate(zip(peers, first)):
            distant = flip(h, peer[1]) - h >= n_head - 1
            if peer[1]:
                due = later(*peer) & (distant == chosen)
            elif chosen:
                continue
            else:
                due = later(*peer)

            @pl.when(due)
            def _(i=i, copy=copy):
                pl.semaphore_wait(ready.at[i], 1)
                copy.start()

    send_later(False)

    def spread(k, d):
        if d == 0:
            for to in reversed(far):
                describe(0, k, p_send.at[k, to // 2], p_recv.at[k, to // 2], to, 0).start()
        describe(d, k, d_send.at[k, d // 2], d_recv.at[k, d // 2], 1, 0).start()

    events = []
    for k in range(n_head):
        for d in range(0, n_seq, 2):
            if d:
                events.append((k + 3 + (bin(d).count("1") - 1) * 0.05, d, k))
            elif k:
                events.append((k, d, k))
    for turn, (_, d, k) in enumerate(sorted(events)):
        if turn == 1:
            send_later(True)
        if d:
            arrived(d, k, p_send.at[k, d // 2], p_recv.at[k, d // 2])
        else:
            arrived(0, k, z_send.at[k - 1], z_recv.at[k - 1])
        spread(k, d)
    for k in range(n_head):
        for d in range(0, n_seq, 2):
            arrived(d + 1, k, d_send.at[k, d // 2], d_recv.at[k, d // 2])
    for copy in sent:
        copy.wait_send()


def attend_kernel(
    dims, order_hbm, queries_ref, kv, table, w_ref, out_ref, q_rows, keys, mixed, state, result, put_sem, order_ref, order_sem
):
    n_seq, n_head, heads, rank, span_len, kv_count, spans_seq = dims
    width = rank + ROPE_DIM
    pairs = heads // 2
    s = lax.axis_index("seq")
    spans = SEQS * spans_seq
    per_span = span_len // kv_count
    rows_all = heads * span_len
    order = pltpu.make_async_copy(order_hbm, order_ref, order_sem)
    order.start()

    def copy_queries(span):
        for par in range(2):
            for pair in range(pairs):
                source = pl.ds(span * span_len, span_len)
                first = pair * 2 * width + par * rank
                rows = pl.ds((pair * 2 + par) * span_len, span_len)
                whole = queries_ref[source, pl.ds(first, rank + LANES)]
                if par:
                    whole = pltpu.roll(whole, rank + LANES - ROPE_DIM, 1)
                q_rows[span, rows, :] = whole

    def rotate_queries(span):
        angles = table[pl.ds(place[span], span_len), :]
        for head in range(heads):
            rows = pl.ds(head * span_len, span_len)
            tail = q_rows[span, rows, rank:].astype(jnp.float32)
            q_rows[span, rows, rank:] = rotate_tile(tail, angles, False).astype(jnp.bfloat16)

    def block_of(stream_span):
        def pick(slot, found):
            return jnp.where(order_ref[slot] == stream_span, slot * per_span, found)

        if spans > 16:
            return lax.fori_loop(0, spans, pick, jnp.int32(0))
        found = jnp.int32(0)
        for slot in range(spans):
            found = pick(slot, found)
        return found

    chunk_spans = min(CHUNK_SPANS, spans_seq)
    n_chunks = spans_seq // chunk_spans
    chunk = chunk_spans * span_len

    def prepare_keys(span, c):
        for j in range(chunk_spans):
            block = block_of(seq_first[span] + c * chunk_spans + j)
            angles = table[pl.ds((c * chunk_spans + j) * span_len, span_len), :]
            rope = []
            for piece in range(per_span):
                rows = pl.ds(j * span_len + piece * kv_count, kv_count)
                for t in range(rank // LANES):
                    keys[span, rows, pl.ds(t * LANES, LANES)] = kv[
                        block + piece, pl.ds(t * kv_count, kv_count), :
                    ]
                tail = kv[block + piece, pl.ds(rank // LANES * kv_count, kv_count // 2), :]
                tail = tail.astype(jnp.float32)
                rope += [tail, pltpu.roll(tail, LANES - ROPE_DIM, 1)]
            rope = rotate_tile(jnp.concatenate(rope, 0), angles, False)
            lane = lax.broadcasted_iota(jnp.int32, rope.shape, 1)
            rows = pl.ds(j * span_len, span_len)
            keys[span, rows, rank:] = jnp.where(lane < ROPE_DIM, rope, 0.0).astype(jnp.bfloat16)

    def one_chunk(span, c):
        limit = lax.broadcasted_iota(jnp.int32, (span_len, chunk), 0) + place[span]
        seen = lax.broadcasted_iota(jnp.int32, (span_len, chunk), 1) + c * chunk <= limit
        for part in range(PARTS):
            share = heads // PARTS
            rows = pl.ds(part * share * span_len, share * span_len)
            scores = (
                lax.dot_general(
                    q_rows[span, rows, :],
                    keys[span],
                    (((1,), (1,)), ((), ())),
                    preferred_element_type=jnp.float32,
                )
                * exponent_scale
            )
            scores = jnp.where(
                seen[None], scores.reshape(share, span_len, chunk), -jnp.inf
            ).reshape(share * span_len, chunk)
            top = jnp.max(scores, 1, keepdims=True)
            if n_chunks > 1:
                old_top = state[rows, 0:1]
                top = jnp.maximum(top, old_top)
                shrink = jnp.exp2(old_top - top)
            expo = jnp.exp2(scores - top)
            total = jnp.sum(expo, 1, keepdims=True)
            sums = jnp.dot(
                expo.astype(jnp.bfloat16),
                keys[span, :, :rank],
                preferred_element_type=jnp.float32,
            )
            if n_chunks > 1:
                total = state[rows, LANES : LANES + 1] * shrink + total
                sums = state[rows, 2 * LANES :] * shrink + sums
                state[rows, :LANES] = jnp.broadcast_to(top, (share * span_len, LANES))
                state[rows, LANES : 2 * LANES] = jnp.broadcast_to(total, (share * span_len, LANES))
                state[rows, 2 * LANES :] = sums
            else:
                finish(span, part * share, share, sums, total)

    def finish(span, first, count, sums, total):
        result = (sums * (1.0 / total)).astype(jnp.bfloat16)
        mixed[pl.ds(first, count), pl.ds(span * span_len, span_len), :] = result.reshape(
            count, span_len, rank
        )

    for span in range(2):
        copy_queries(span)
    order.wait()
    seq_first, place = span_places(order_ref, s, spans_seq, span_len)
    for span in range(2):
        rotate_queries(span)
        if n_chunks == 1:
            prepare_keys(span, 0)
            one_chunk(span, 0)
        else:
            state[:, :LANES] = jnp.full((rows_all, LANES), -1e30, jnp.float32)
            state[:, LANES:] = jnp.zeros((rows_all, LANES + rank), jnp.float32)

            @pl.loop(0, n_chunks)
            def _(c, span=span):
                prepare_keys(span, c)
                one_chunk(span, c)

            finish(span, 0, heads, state[:, 2 * LANES :], state[:, LANES : LANES + 1])

    v_dim = w_ref.shape[2]
    puts = []
    for part in range(PUTS):
        share = heads // PUTS
        for head in range(part * share, part * share + share):
            result[:, pl.ds(head * v_dim, v_dim)] = jnp.dot(
                mixed[head], w_ref[head], preferred_element_type=jnp.float32
            ).astype(jnp.bfloat16)
        lanes = pl.ds(part * share * v_dim, share * v_dim)
        puts.append(pltpu.make_async_copy(result.at[:, lanes], out_ref.at[:, lanes], put_sem.at[part]))
        puts[-1].start()
    for put in puts:
        put.wait()


def per_device(n_seq, n_head, span_order, queries, latent_kv, w_uv):
    tok_dev = queries.shape[0]
    heads, rank, v_dim = w_uv.shape
    kv_count, width = latent_kv.shape
    span_len = tok_dev // 2
    spans = span_order.shape[0]
    spans_seq = spans // SEQS
    seq_len = spans_seq * span_len
    wide = rank + LANES
    packed = kv_count * width // LANES
    chunk_spans = min(CHUNK_SPANS, spans_seq)
    state_rows = heads * span_len if spans_seq > chunk_spans else 8
    dims = (n_seq, n_head, heads, rank, span_len, kv_count, spans_seq)
    table = jnp.asarray(angle_table(seq_len, ROPE_DIM // 2))
    dma = pltpu.SemaphoreType.DMA
    vmem = pl.BlockSpec(memory_space=pltpu.VMEM)
    kv = pl.pallas_call(
        functools.partial(gather_kernel, dims),
        out_shape=jax.ShapeDtypeStruct((n_seq * n_head, packed, LANES), jnp.bfloat16),
        in_specs=[vmem],
        out_specs=vmem,
        scratch_shapes=[
            dma((max(n_head - 1, 1),)),
            dma((max(n_head - 1, 1),)),
            dma((n_head, n_seq // 2)),
            dma((n_head, n_seq // 2)),
            dma((n_head, n_seq // 2)),
            dma((n_head, n_seq // 2)),
            pltpu.SemaphoreType.REGULAR((n_head + n_seq // 2 - 1,)),
        ],
        compiler_params=pltpu.CompilerParams(
            collective_id=0, has_side_effects=True, vmem_limit_bytes=GATHER_MIB << 20
        ),
        cost_estimate=pl.CostEstimate(flops=20 << 30, bytes_accessed=1 << 20, transcendentals=0),
        name="gather_keys",
    )(latent_kv)
    return pl.pallas_call(
        functools.partial(attend_kernel, dims),
        out_shape=jax.ShapeDtypeStruct((tok_dev, heads * v_dim), jnp.bfloat16),
        in_specs=[pl.BlockSpec(memory_space=pl.ANY), vmem, vmem, vmem, vmem],
        out_specs=pl.BlockSpec(memory_space=pl.ANY),
        scratch_shapes=[
            pltpu.VMEM((2, heads * span_len, wide), jnp.bfloat16),
            pltpu.VMEM((2, chunk_spans * span_len, wide), jnp.bfloat16),
            pltpu.VMEM((heads, tok_dev, rank), jnp.bfloat16),
            pltpu.VMEM((state_rows, 2 * LANES + rank), jnp.float32),
            pltpu.VMEM((tok_dev, heads * v_dim), jnp.bfloat16),
            dma((PUTS,)),
            pltpu.SMEM(span_order.shape, jnp.int32),
            dma,
        ],
        compiler_params=pltpu.CompilerParams(vmem_limit_bytes=ATTEND_MIB << 20),
        cost_estimate=pl.CostEstimate(flops=4 << 30, bytes_accessed=8 << 20, transcendentals=1 << 20),
        name="attend",
    )(span_order, queries, kv, table, w_uv)


def solution(mesh):
    in_specs = (P(), P("seq", "head"), P(("seq", "head"), None), P("head", None, None))
    return jax.shard_map(
        functools.partial(per_device, mesh.shape["seq"], mesh.shape["head"]),
        mesh=mesh,
        in_specs=in_specs,
        out_specs=P("seq", "head"),
        check_vma=False,
    )
```
